1024 devices in a mesh: tp: 64 (over y, x), dp: 16 (over z, core).
Axes of the slice: x: 8, y: 8, z: 8, core: 2. Of those that a mesh axis runs over, the one named last changes fastest.
Arguments:
- grad_out: bfloat16 [2048, 16384], P('dp', 'tp'), may hold values from -6 to 6
- hidden_sum: bfloat16 [2048, 16384], P('dp', 'tp'), may hold values from -100 to 100
- norm_gain: float32 [16384], P('tp'), may hold values from 0.5 to 1.5
- out_weight: bfloat16 [16384, 16384], P(None, 'tp'), may hold values from -0.046875 to 0.046875
Outputs:
- resid_grad: bfloat16 [2048, 16384], P('dp', 'tp')
- attn_grad: bfloat16 [2048, 16384], P('dp', 'tp')
- gain_grad: float32 [16384], P('tp')
The draws below stay inside these ranges and needn't reach their ends.
All inputs are finite; a program needn't handle non-finite values.
Results may differ from the reference program's by a relative error of at most 0.0049.
Values sent between devices are 32-bit elements; how exact they have to be, the bound alone decides.
A program may use at most 64 MiB of HBM per device.

```python
import math
import jax
import jax.numpy as jnp
from jax import lax

D = 16384
TOKENS = 2048
D_IN = 16384


def draw_hidden_sum(key, part):
    key_values, key_row, key_col = jax.random.split(jax.random.fold_in(key, 11), 3)
    position = jnp.arange(D, dtype=jnp.float32) / D
    column = jnp.exp(math.log(3.0) * position + math.log(10.0) * jax.random.uniform(key_col, (D,), jnp.float32))
    column = column / jnp.sqrt(jnp.mean(column * column))
    values = jnp.clip(jax.random.normal(key_values, (TOKENS, D), jnp.float32), -4.0, 4.0)
    row_scale = jnp.exp(jax.random.uniform(key_row, (TOKENS, 1), jnp.float32, minval=math.log(0.3), maxval=math.log(3.0)))
    return jnp.clip(values * row_scale * column, -100.0, 100.0).astype(jnp.bfloat16)


def steps_of(own_key, dims, cuts, low, largest):
    level = 1.0
    for dim, blocks in cuts:
        steps = jax.random.uniform(jax.random.fold_in(jax.random.fold_in(own_key, 6), dim), (blocks,), jnp.float32, low / len(cuts), largest / len(cuts))
        level = level * jnp.repeat(jnp.exp(steps), dims[dim] // blocks).reshape((-1,) + (1,) * (len(dims) - 1 - dim))
    return level


def normal_values(own_key, dims, deviation, most, cuts=(), kind=jnp.bfloat16):
    array = deviation * jax.random.normal(own_key, dims, jnp.float32)
    if cuts:
        array = array * steps_of(own_key, dims, cuts, -0.22, 0.18)
    return jnp.clip(array, -most, most).astype(kind)


def setup_inputs(seed: int = 0) -> dict:
    seeds = jax.random.split(jax.random.key(seed), 5)
    grad_out = normal_values(seeds[0], (TOKENS, D), 1.0, 6.0, ((0, 16), (1, 64)))
    hidden_sum = draw_hidden_sum(jax.random.fold_in(seeds[4], 71), 0)
    norm_gain = jnp.clip(0.5 + 1.0 * jax.random.uniform(seeds[2], (D,), jnp.float32) ** steps_of(seeds[2], (D,), ((0, 64),), -0.2, 0.2), 0.5, 1.5)
    out_weight = normal_values(seeds[3], (D_IN, D), D ** -0.5, 0.046875, ((1, 64),))
    return dict(grad_out=grad_out, hidden_sum=hidden_sum, norm_gain=norm_gain, out_weight=out_weight)


epsilon = 1e-05

def backward_rows(upstream_b, stream_b, norm_gain, out_weight):
    upstream = upstream_b.astype(jnp.float32)
    stream = stream_b.astype(jnp.float32)
    squares = lax.optimization_barrier(jnp.sum(stream * stream, axis=1))
    inverse = lax.rsqrt(squares / D + epsilon)
    dotted = lax.optimization_barrier(jnp.sum(norm_gain * upstream * stream, axis=1))
    factor = inverse * inverse * dotted / D
    resid_full = inverse[:, None] * (norm_gain * upstream - stream * factor[:, None])
    resid_grad = resid_full.astype(jnp.bfloat16)
    attn_grad = jnp.dot(resid_grad, out_weight.T, preferred_element_type=jnp.float32).astype(jnp.bfloat16)
    gain_part = lax.optimization_barrier(jnp.sum(upstream * stream * inverse[:, None], axis=0))
    return (resid_grad, attn_grad, gain_part)

def reference(grad_out, hidden_sum, norm_gain, out_weight):
    span_rows = math.gcd(TOKENS, 512)
    number = TOKENS // span_rows

    def advance(carry, pieces):
        resid_grad, attn_grad, gain_part = backward_rows(pieces[0], pieces[1], norm_gain, out_weight)
        return (carry + gain_part, (resid_grad, attn_grad))
    gain_grad, outputs = lax.scan(advance, jnp.zeros((D,), jnp.float32), (grad_out.reshape(number, span_rows, D), hidden_sum.reshape(number, span_rows, D)))
    return (outputs[0].reshape(TOKENS, D), outputs[1].reshape(TOKENS, D_IN), gain_grad)
```

```python
import functools

import jax
import jax.numpy as jnp
from jax import lax
from jax.experimental import pallas as pl
from jax.experimental.pallas import tpu as pltpu
from jax.sharding import Mesh
from jax.sharding import PartitionSpec as P

EPSILON = 1e-05
MESH = pl.DeviceIdType.MESH
LOADS = 4


def kernel(
    n, width,
    grad_hbm, stream_hbm, gain_hbm, weight_hbm,
    resid_out, attn_out, gain_out,
    grad_v, stream_v, gain_v, weight_v,
    scaled_t, stream_t, resid_t, operand, inverse_v,
    stat, stat_in, part, ring, turn, tail, final_t, gains,
    load_sem, stat_send, stat_recv, ring_send, ring_recv, tail_send, tail_recv, gain_send, gain_recv,
):
    y, x = lax.axis_index("y"), lax.axis_index("x")
    z, core = lax.axis_index("z"), lax.axis_index("core")
    half = n // 2
    here = {"x": x, "y": y}
    first_axis, second_axis = ("x", "y"), ("y", "x")
    rows = part.shape[-2]
    tokens = part.shape[-1]
    halved = rows // 2

    small = [
        pltpu.make_async_copy(s, d, load_sem.at[i])
        for i, (s, d) in enumerate(((grad_hbm, grad_v), (stream_hbm, stream_v), (gain_hbm, gain_v)))
    ]
    for load in small:
        load.start()
    span = weight_v.shape[0] // LOADS
    big = [
        pltpu.make_async_copy(
            weight_hbm.at[pl.ds(i * span, span)], weight_v.at[pl.ds(i * span, span)], load_sem.at[3 + i]
        )
        for i in range(LOADS)
    ]
    for load in big:
        load.start()

    zs = lax.axis_size("z")
    flips, bit = [{"core": 1 - core}], 1
    while bit < zs:
        flips.append({"z": z + bit - 2 * bit * lax.rem(z // bit, 2)})
        bit *= 2
    barrier = pltpu.get_barrier_semaphore()
    peers = [{a: lax.rem(here[a] + j, n)} for a in ("x", "y") for j in range(1, n)] + flips
    for peer in peers:
        pl.semaphore_signal(barrier, inc=1, device_id=peer, device_id_type=MESH)

    for load in small:
        load.wait()
    grad = grad_v[...].astype(jnp.float32)
    stream = stream_v[...].astype(jnp.float32)
    scaled_t[...] = jnp.transpose(gain_v[...] * grad)
    stream_t[...] = jnp.transpose(stream)
    stat[...] = jnp.zeros_like(stat)
    stat[0, 0:1, :] = jnp.sum(stream_t[...] * stream_t[...], axis=0, keepdims=True)
    stat[0, 1:2, :] = jnp.sum(scaled_t[...] * stream_t[...], axis=0, keepdims=True)
    pl.semaphore_wait(barrier, len(peers))

    def stat_copy(a, j):
        axis = ("x", "y")[a]
        return pltpu.make_async_remote_copy(
            src_ref=stat.at[a], dst_ref=stat_in.at[a, j],
            send_sem=stat_send.at[a, j], recv_sem=stat_recv.at[a, j],
            device_id={axis: lax.rem(here[axis] + j, n)}, device_id_type=MESH,
        )

    far_first = sorted(range(1, n), key=lambda j: -min(j, n - j))
    for a in range(2):
        for j in far_first:
            stat_copy(a, j).start()
        for j in reversed(far_first):
            stat_copy(a, j).wait_recv()
        both = stat[a]
        for j in range(1, n):
            both = both + stat_in[a, j]
        if a == 0:
            stat[1] = both
    inverse = lax.rsqrt(both[0:1] / width + EPSILON)
    factor = inverse * inverse * both[1:2] / width
    inverse_v[...] = jnp.broadcast_to(inverse, inverse_v.shape)
    resid = inverse * (scaled_t[...] - stream_t[...] * factor)
    resid_t[...] = resid
    operand[...] = resid.astype(jnp.bfloat16)
    for load in big:
        load.wait()

    def offset(c):
        return lax.rem(lax.select(lax.rem(c, 2) == 1, (n - 1 - c) // 2, half + c // 2), n)

    def multiply(c):
        o = offset(c)
        for h in range(2):
            for j in range(n):
                if h == 0:
                    yy, xx = lax.rem(y + o, n), lax.rem(x + j, n)
                else:
                    yy, xx = lax.rem(y + j, n), lax.rem(x + o, n)
                part[h, c, j] = jnp.dot(
                    weight_v[(yy * n + xx) * 2 + h], operand[...], preferred_element_type=jnp.float32
                )

    def side(d):
        return pl.ds(d * halved, halved)

    def ring_copy(h, d, c, s):
        axis = first_axis[h]
        if s == 1:
            src, dst = part.at[h, c, half, side(d)], ring.at[h, d, c, 0, side(d)]
        else:
            src, dst = ring.at[h, d, c, s - 2], ring.at[h, d, c, s - 1]
        return pltpu.make_async_remote_copy(
            src_ref=src, dst_ref=dst,
            send_sem=ring_send.at[h, d, c, s - 1], recv_sem=ring_recv.at[h, d, c, s - 1],
            device_id={axis: lax.rem(here[axis] + (1 if d == 0 else n - 1), n)}, device_id_type=MESH,
        )

    def tail_copy(h, d, s, last=False):
        axis = second_axis[h]
        if isinstance(s, int) and s == 1:
            src, dst = turn.at[h, side(d)], tail.at[h, d, 0, side(d)]
        else:
            src, dst = tail.at[h, d, s - 2], tail.at[h, d, s - 1]
        return pltpu.make_async_remote_copy(
            src_ref=src, dst_ref=dst,
            send_sem=tail_send.at[h, d, s - 1], recv_sem=tail_recv.at[h, d, s - 1],
            device_id={axis: lax.rem(here[axis] + 1 + d * (n - 2), n)}, device_id_type=MESH,
        )

    def begin(c):
        multiply(c)
        for h in range(2):
            for d in range(2):
                ring_copy(h, d, c, 1).start()

    def add(slot, other, d, s):
        if s == 1:
            slot[side(d)] += other[side(d)]
            slot[side(1 - d)] = other[side(1 - d)]
        else:
            slot[...] += other[...]

    def pass_on(c, s):
        m = half + 1 - s
        for h in range(2):
            for d in range(2):
                ring_copy(h, d, c, s - 1).wait_recv()
                add(ring.at[h, d, c, s - 2], part.at[h, c, m if d == 0 else n - m], d, s - 1)
                ring_copy(h, d, c, s).start()

    def sends_done(c):
        for h in range(2):
            for d in range(2):
                for s in range(1, half + 1):
                    ring_copy(h, d, c, s).wait_send()

    def arrive(c):
        for h in range(2):
            for d in range(2):
                ring_copy(h, d, c, half).wait_recv()
            turn_value = ring[h, 0, c, half - 1] + ring[h, 1, c, half - 1] + part[h, c, 0]

            @pl.when(c == 0)
            def _():
                turn[h] = turn_value
                for d in range(2):
                    tail_copy(h, d, 1).start()

            d = 1 - lax.rem(c, 2)
            for s in range(2, half + 1):

                @pl.when((c > 0) & ((c + 1) // 2 + 1 == s) & (c < n - 1))
                def _():
                    tail_copy(h, d, s - 1).wait_recv()
                    slot = tail.at[h, d, s - 2]
                    if s == 2:
                        other = pl.ds((1 - d) * halved, halved)
                        part[h, c, 0] = turn_value
                        slot[side(d)] += part[h, c, 0, side(d)]
                        slot[other] = part[h, c, 0, other]
                    else:
                        slot[...] += turn_value
                    tail_copy(h, d, s).start()

            @pl.when(c == n - 1)
            def _():
                for d in range(2):
                    tail_copy(h, d, half).wait_recv()
                final_t[h] = turn_value + tail[h, 0, half - 1] + tail[h, 1, half - 1]

    def gain_copy(k):
        return pltpu.make_async_remote_copy(
            src_ref=gains.at[0, k], dst_ref=gains.at[1, k],
            send_sem=gain_send.at[k], recv_sem=gain_recv.at[k],
            device_id=flips[k], device_id_type=MESH,
        )

    def aside(t):
        lanes = tokens

        @pl.when(t == 2)
        def _():
            column = jnp.transpose(jnp.broadcast_to(inverse_v[0:1], (tokens, tokens)))
            gains[0, 0] = jnp.zeros_like(gains[0, 0])
            for i in range(grad_v.shape[1] // lanes):
                at = pl.ds(i * lanes, lanes)
                product = grad_v[:, at].astype(jnp.float32) * stream_v[:, at].astype(jnp.float32) * column
                gains[0, 0, 0:1, at] = jnp.sum(product, axis=0, keepdims=True)
            gain_copy(0).start()

        for k in range(1, len(flips) + 1):

            @pl.when(t == 2 + k)
            def _():
                gain_copy(k - 1).wait_recv()
                total = gains[0, k - 1] + gains[1, k - 1]
                if k < len(flips):
                    gains[0, k] = total
                    gain_copy(k).start()
                else:
                    gain_out[...] = total[0:1]

        @pl.when(t == 1)
        def _():
            resid_out[...] = jnp.transpose(resid_t[...]).astype(jnp.bfloat16)

    begin(0)
    begin(1)

    def slot(t, _):
        @pl.when(t + 2 < n)
        def _():
            begin(t + 2)

        for s in range(2, half + 1):
            c = t - (s - 2)

            @pl.when((c >= 0) & (c < n))
            def _():
                pass_on(c, s)

        c = t - (half - 1)

        @pl.when((c >= 0) & (c < n))
        def _():
            arrive(c)

        @pl.when((c >= 1) & (c < n))
        def _():
            sends_done(c - 1)

        aside(t)
        return 0

    slots = n + half - 1
    assert slots > 2 + len(flips)
    lax.fori_loop(0, slots, slot, 0)

    for h in range(2):
        attn_out[:, pl.ds(h * rows, rows)] = jnp.transpose(final_t[h]).astype(jnp.bfloat16)

    sends_done(n - 1)
    for h in range(2):
        for d in range(2):
            for s in range(1, half + 1):
                tail_copy(h, d, s).wait_send()
    for k in range(len(flips)):
        gain_copy(k).wait_send()
    for a in range(2):
        for j in range(1, n):
            stat_copy(a, j).wait_send()


def on_device(n, zs, width, grad_out, hidden_sum, norm_gain, out_weight):
    tokens, features = grad_out.shape
    rows = features // 2
    half = n // 2
    groups = out_weight.shape[0] // rows
    flips = 1 + (zs - 1).bit_length()
    f32, bf16 = jnp.float32, jnp.bfloat16
    block = (rows, tokens)
    resid, attn, gains = pl.pallas_call(
        functools.partial(kernel, n, width),
        out_shape=(
            jax.ShapeDtypeStruct((tokens, features), bf16),
            jax.ShapeDtypeStruct((tokens, features), bf16),
            jax.ShapeDtypeStruct((1, features), f32),
        ),
        in_specs=[pl.BlockSpec(memory_space=pl.ANY)] * 4,
        out_specs=(pl.BlockSpec(memory_space=pltpu.VMEM),) * 3,
        scratch_shapes=[
            pltpu.VMEM((tokens, features), bf16),
            pltpu.VMEM((tokens, features), bf16),
            pltpu.VMEM((1, features), f32),
            pltpu.VMEM((groups, rows, features), bf16),
            pltpu.VMEM((features, tokens), f32),
            pltpu.VMEM((features, tokens), f32),
            pltpu.VMEM((features, tokens), f32),
            pltpu.VMEM((features, tokens), bf16),
            pltpu.VMEM((8, tokens), f32),
            pltpu.VMEM((2, 8, tokens), f32),
            pltpu.VMEM((2, n, 8, tokens), f32),
            pltpu.VMEM((2, n, n) + block, f32),
            pltpu.VMEM((2, 2, n, half) + block, f32),
            pltpu.VMEM((2,) + block, f32),
            pltpu.VMEM((2, 2, half) + block, f32),
            pltpu.VMEM((2,) + block, f32),
            pltpu.VMEM((2, flips, 8, features), f32),
            pltpu.SemaphoreType.DMA((3 + LOADS,)),
            pltpu.SemaphoreType.DMA((2, n)),
            pltpu.SemaphoreType.DMA((2, n)),
            pltpu.SemaphoreType.DMA((2, 2, n, half)),
            pltpu.SemaphoreType.DMA((2, 2, n, half)),
            pltpu.SemaphoreType.DMA((2, 2, half)),
            pltpu.SemaphoreType.DMA((2, 2, half)),
            pltpu.SemaphoreType.DMA((flips,)),
            pltpu.SemaphoreType.DMA((flips,)),
        ],
        compiler_params=pltpu.CompilerParams(
            collective_id=0, has_side_effects=True, vmem_limit_bytes=48 * 1024 * 1024
        ),
        name="fused",
    )(grad_out, hidden_sum, norm_gain.reshape(1, features), out_weight.reshape(groups, rows, features))
    return resid, attn, gains.reshape(features)


def solution(mesh, n=8, zs=8):
    finer = Mesh(mesh.devices.reshape(n, n, zs, 2), ("y", "x", "z", "core"))
    tp, dp = ("y", "x"), ("z", "core")

    def whole(grad_out, hidden_sum, norm_gain, out_weight):
        return jax.shard_map(
            functools.partial(on_device, n, zs, grad_out.shape[1]),
            mesh=finer,
            in_specs=(P(dp, tp), P(dp, tp), P(tp), P(None, tp)),
            out_specs=(P(dp, tp), P(dp, tp), P(tp)),
            check_vma=False,
        )(grad_out, hidden_sum, norm_gain, out_weight)

    return whole
```

```python
import functools

import jax
import jax.numpy as jnp
from jax import lax
from jax.experimental import pallas as pl
from jax.experimental.pallas import tpu as pltpu
from jax.sharding import Mesh
from jax.sharding import PartitionSpec as P

EPSILON = 1e-05
MESH = pl.DeviceIdType.MESH
EARLY = 2


def kernel(
    n, width,
    grad_hbm, stream_hbm, gain_hbm, weight_hbm,
    out, gain_out,
    grad_v, stream_v, gain_v, weight_v,
    scaled_t, stream_t, resid_t, operand, early, token_v,
    stat, stat_in, early_part, early_ring, part, ring, turn, tail, final_t, gains,
    load_sem, stat_send, stat_recv, early_send, early_recv, ring_send, ring_recv, tail_send, tail_recv, gain_send, gain_recv, entered,
):
    y, x = lax.axis_index("y"), lax.axis_index("x")
    z, core = lax.axis_index("z"), lax.axis_index("core")
    half = n // 2
    here = {"x": x, "y": y}
    first_axis, second_axis = ("x", "y"), ("y", "x")
    rows = part.shape[-2]
    tokens = part.shape[-1]
    halved = rows // 2

    small = [
        pltpu.make_async_copy(s, d, load_sem.at[i])
        for i, (s, d) in enumerate(((grad_hbm, grad_v), (stream_hbm, stream_v), (gain_hbm, gain_v)))
    ]
    for load in small:
        load.start()
    def offset(c):
        c = jnp.int32(c)
        return lax.rem(lax.select(lax.rem(c, 2) == 1, (n - 1 - c) // 2, half + c // 2), n)

    def weight_load(h, c):
        i = lax.rem(here[second_axis[h]] + offset(c), n)
        return pltpu.make_async_copy(
            weight_hbm.at[i, :, 0] if h == 0 else weight_hbm.at[:, i, 1], weight_v.at[h, i], load_sem.at[3 + h * n + c]
        )

    for c in range(n):
        for h in range(2):
            weight_load(h, c).start()

    zs = lax.axis_size("z")
    flips, uppers, bit = [{"core": 1 - core}], [], 1
    while bit < zs:
        upper = lax.rem(z // bit, 2)
        flips.append({"z": z + bit - 2 * bit * upper})
        uppers.append(upper)
        bit *= 2
    barrier = pltpu.get_barrier_semaphore()
    peers = [{a: lax.rem(here[a] + j, n)} for a in ("x", "y") for j in range(1, n)] + flips[:1]
    for peer in peers:
        pl.semaphore_signal(barrier, inc=1, device_id=peer, device_id_type=MESH)
    for k, upper in enumerate(uppers):

        @pl.when(upper == 0)
        def _():
            pl.semaphore_signal(barrier, inc=1, device_id=flips[1 + k], device_id_type=MESH)

    for load in small:
        load.wait()
    grad = grad_v[...].astype(jnp.float32)
    stream = stream_v[...].astype(jnp.float32)
    scaled_t[...] = jnp.transpose(gain_v[...] * grad)
    stream_t[...] = jnp.transpose(stream)
    stat[0, 0:1, :] = jnp.sum(stream_t[...] * stream_t[...], axis=0, keepdims=True)
    stat[0, 1:2, :] = jnp.sum(scaled_t[...] * stream_t[...], axis=0, keepdims=True)
    scaled = scaled_t[...]
    high = scaled.astype(jnp.bfloat16)
    early[0] = high
    early[1] = (scaled - high.astype(jnp.float32)).astype(jnp.bfloat16)
    early[2] = stream_t[...].astype(jnp.bfloat16)
    pl.semaphore_wait(barrier, len(peers) + sum(uppers))

    def stat_copy(a, j):
        axis = ("x", "y")[a]
        return pltpu.make_async_remote_copy(
            src_ref=stat.at[a], dst_ref=stat_in.at[a, j],
            send_sem=stat_send.at[a, j], recv_sem=stat_recv.at[a, j],
            device_id={axis: lax.rem(here[axis] + j, n)}, device_id_type=MESH,
        )

    def spot(h, j):
        return lax.rem(here[first_axis[h]] + j, n)

    def slab(h, o):
        blocks = weight_v[h, lax.rem(here[second_axis[h]] + o, n)]
        return blocks.reshape(n * rows, blocks.shape[-1])

    def product(a, b):
        return jnp.dot(a, b, preferred_element_type=jnp.float32)

    def multiply(c):
        for h in range(2):
            part[h, c] = product(slab(h, offset(c)), operand[...]).reshape(n, rows, tokens)

    def multiply_early(c):
        for h in range(2):
            blocks = slab(h, offset(c))
            value = product(blocks, early[0]) + product(blocks, early[1])
            early_part[h, c, 0] = value.reshape(n, rows, tokens)
            early_part[h, c, 1] = product(blocks, early[2]).reshape(n, rows, tokens)

    def side(d):
        return pl.ds(d * halved, halved)

    def ring_copy(h, d, c, s):
        axis = first_axis[h]
        if s == 1:
            src, dst = part.at[h, c, spot(h, half), side(d)], ring.at[h, d, c, 0, side(d)]
        else:
            src, dst = ring.at[h, d, c, s - 2], ring.at[h, d, c, s - 1]
        return pltpu.make_async_remote_copy(
            src_ref=src, dst_ref=dst,
            send_sem=ring_send.at[h, d, c, s - 1], recv_sem=ring_recv.at[h, d, c, s - 1],
            device_id={axis: lax.rem(here[axis] + (1 if d == 0 else n - 1), n)}, device_id_type=MESH,
        )

    def tail_copy(h, d, s, last=False):
        axis = second_axis[h]
        if isinstance(s, int) and s == 1:
            src, dst = turn.at[h, side(d)], tail.at[h, d, 0, side(d)]
        else:
            src, dst = tail.at[h, d, s - 2], tail.at[h, d, s - 1]
        return pltpu.make_async_remote_copy(
            src_ref=src, dst_ref=dst,
            send_sem=tail_send.at[h, d, s - 1], recv_sem=tail_recv.at[h, d, s - 1],
            device_id={axis: lax.rem(here[axis] + 1 + d * (n - 2), n)}, device_id_type=MESH,
        )

    def begin(c):
        multiply(c)
        for h in range(2):
            for d in range(2):
                ring_copy(h, d, c, 1).start()

    def early_copy(h, d, c, g, s):
        axis = first_axis[h]
        if s == 1:
            src, dst = early_part.at[h, c, g, spot(h, half), side(d)], early_ring.at[h, d, c, g, 0, side(d)]
        else:
            src, dst = early_ring.at[h, d, c, g, 0], early_ring.at[h, d, c, g, 1]
        return pltpu.make_async_remote_copy(
            src_ref=src, dst_ref=dst,
            send_sem=early_send.at[h, d, c, g, s - 1], recv_sem=early_recv.at[h, d, c, g, s - 1],
            device_id={axis: lax.rem(here[axis] + (1 if d == 0 else n - 1), n)}, device_id_type=MESH,
        )

    def begin_early(c):
        multiply_early(c)
        for g in range(2):
            for h in range(2):
                for d in range(2):
                    early_copy(h, d, c, g, 1).start()

    def add(slot, other, d, s):
        if s == 1:
            slot[side(d)] += other[side(d)]
            slot[side(1 - d)] = other[side(1 - d)]
        else:
            slot[...] += other[...]

    def ahead(d, s):
        m = half + 1 - s
        return m if d == 0 else n - m

    def pass_on(c, s):
        for h in range(2):
            for d in range(2):
                ring_copy(h, d, c, s - 1).wait_recv()
                add(ring.at[h, d, c, s - 2], part.at[h, c, spot(h, ahead(d, s))], d, s - 1)
                ring_copy(h, d, c, s).start()

    def pass_early(c):
        for g in range(2):
            for h in range(2):
                for d in range(2):
                    early_copy(h, d, c, g, 1).wait_recv()
                    add(early_ring.at[h, d, c, g, 0], early_part.at[h, c, g, spot(h, ahead(d, 2))], d, 1)
                    early_copy(h, d, c, g, 2).start()

    def join_early(c):
        multiply(c)
        for h in range(2):
            for d in range(2):
                for g in range(2):
                    early_copy(h, d, c, g, 2).wait_recv()
                joined = early_ring[h, d, c, 0, 1] - early_ring[h, d, c, 1, 1] * token_v[1, 0:1]
                ring[h, d, c, 1] = token_v[0, 0:1] * joined + part[h, c, spot(h, ahead(d, 3))]
                ring_copy(h, d, c, 3).start()

    def sends_done(c, first=1):
        for h in range(2):
            for d in range(2):
                for s in range(first, half + 1):
                    ring_copy(h, d, c, s).wait_send()

    def gathered(h, e):
        for d in range(2):
            ring_copy(h, d, e, half).wait_recv()
        return ring[h, 0, e, half - 1] + ring[h, 1, e, half - 1] + part[h, e, spot(h, 0)]

    def turn_first():
        for h in range(2):
            turn[h] = gathered(h, 0)
            for d in range(2):
                tail_copy(h, d, 1).start()

    def arrive(c):
        for h in range(2):
            turn_value = gathered(h, c)
            d = 1 - lax.rem(c, 2)
            for s in range(2, half + 1):

                @pl.when(((c + 1) // 2 + 1 == s) & (c < n - 1))
                def _():
                    tail_copy(h, d, s - 1).wait_recv()
                    slot = tail.at[h, d, s - 2]
                    if s == 2:
                        other = pl.ds((1 - d) * halved, halved)
                        mine = part.at[h, c, spot(h, 0)]
                        mine[...] = turn_value
                        slot[side(d)] += mine[side(d)]
                        slot[other] = mine[other]
                    else:
                        slot[...] += turn_value
                    tail_copy(h, d, s).start()

            @pl.when(c == n - 1)
            def _():
                for d in range(2):
                    tail_copy(h, d, half).wait_recv()
                final_t[h] = turn_value + tail[h, 0, half - 1] + tail[h, 1, half - 1]

    def gain_copy(k):
        return pltpu.make_async_remote_copy(
            src_ref=gains.at[0, k], dst_ref=gains.at[1, k],
            send_sem=gain_send.at[k], recv_sem=gain_recv.at[k],
            device_id=flips[k], device_id_type=MESH,
        )

    def write_resid():
        out[0:tokens] = jnp.transpose(resid_t[...]).astype(out.dtype)

    def gain_first():
        column = jnp.transpose(jnp.broadcast_to(token_v[0, 0:1], (tokens, tokens)))
        gains[0, 0] = jnp.zeros_like(gains[0, 0])
        for i in range(grad_v.shape[1] // tokens):
            at = pl.ds(i * tokens, tokens)
            value = grad_v[:, at].astype(jnp.float32) * stream_v[:, at].astype(jnp.float32) * column
            gains[0, 0, 0:1, at] = jnp.sum(value, axis=0, keepdims=True)
        gain_copy(0).start()

    def gain_step(k):
        gain_copy(k - 1).wait_recv()
        gains[0, k] = gains[0, k - 1] + gains[1, k - 1]

        @pl.when(uppers[k - 1] == 0)
        def _():
            pl.semaphore_wait(entered.at[k - 1], 1)

        gain_copy(k).start()

    def send_stats(a):
        for j in sorted(range(1, n), key=lambda j: -min(j, n - j)):
            stat_copy(a, j).start()

    def take_stats(a):
        for j in sorted(range(1, n), key=lambda j: min(j, n - j)):
            stat_copy(a, j).wait_recv()
        both = stat[a]
        for j in range(1, n):
            both = both + stat_in[a, j]
        return both

    send_stats(0)
    for k, upper in enumerate(uppers):

        @pl.when(upper == 1)
        def _():
            pl.semaphore_signal(entered.at[k], inc=1, device_id=flips[1 + k], device_id_type=MESH)

    for c in range(EARLY):
        for h in range(2):
            weight_load(h, c).wait()
        begin_early(c)
    for c in range(EARLY, n):
        for h in range(2):
            weight_load(h, c).wait()
    stat[1] = take_stats(0)
    send_stats(1)
    middle = EARLY + (n - EARLY) // 2
    front, back = (EARLY, middle), (middle, n)

    def each(chunks, do):
        lax.fori_loop(chunks[0], chunks[1], lambda c, _: (do(c), 0)[1], 0)

    for c in range(EARLY):
        pass_early(c)
    both = take_stats(1)
    inverse = lax.rsqrt(both[0:1] / width + EPSILON)
    factor = inverse * inverse * both[1:2] / width
    token_v[0] = jnp.broadcast_to(inverse, token_v.shape[1:])
    token_v[1] = jnp.broadcast_to(factor, token_v.shape[1:])
    resid = inverse * (scaled_t[...] - stream_t[...] * factor)
    resid_t[...] = resid
    operand[...] = resid.astype(jnp.bfloat16)

    each(front, begin)
    gain_first()
    each((0, EARLY), join_early)
    gain_step(1)
    each(front, lambda c: pass_on(c, 2))
    each((0, EARLY), lambda c: pass_on(c, 4))
    gain_step(2)
    each(front, lambda c: pass_on(c, 3))
    turn_first()
    each(back, begin)
    each(front, lambda c: pass_on(c, 4))
    gain_step(3)
    write_resid()
    each((1, 3), arrive)
    each(back, lambda c: pass_on(c, 2))
    each((3, 5), arrive)
    each(back, lambda c: pass_on(c, 3))
    each((0, EARLY), lambda c: sends_done(c, 3))
    each(front, sends_done)
    each(back, lambda c: pass_on(c, 4))
    each((5, n), arrive)

    for h in range(2):
        out[pl.ds(tokens, tokens), pl.ds(h * rows, rows)] = jnp.transpose(final_t[h]).astype(out.dtype)
    last = len(flips) - 1
    gain_copy(last).wait_recv()
    gain_out[...] = (gains[0, last] + gains[1, last])[0:1]

    each(back, sends_done)
    for h in range(2):
        for d in range(2):
            for c in range(EARLY):
                for g in range(2):
                    for s in range(1, 3):
                        early_copy(h, d, c, g, s).wait_send()
    for h in range(2):
        for d in range(2):
            for s in range(1, half + 1):
                tail_copy(h, d, s).wait_send()
    for k in range(len(flips)):
        gain_copy(k).wait_send()
    for a in range(2):
        for j in range(1, n):
            stat_copy(a, j).wait_send()


def on_device(n, zs, width, grad_out, hidden_sum, norm_gain, out_weight):
    tokens, features = grad_out.shape
    rows = features // 2
    half = n // 2
    flips = 1 + (zs - 1).bit_length()
    f32, bf16 = jnp.float32, jnp.bfloat16
    block = (rows, tokens)
    out, gains = pl.pallas_call(
        functools.partial(kernel, n, width),
        out_shape=(
            jax.ShapeDtypeStruct((2 * tokens, features), bf16),
            jax.ShapeDtypeStruct((1, features), f32),
        ),
        in_specs=[pl.BlockSpec(memory_space=pltpu.HBM)] * 4,
        out_specs=(pl.BlockSpec(memory_space=pltpu.VMEM),) * 2,
        scratch_shapes=[
            pltpu.VMEM((tokens, features), bf16),
            pltpu.VMEM((tokens, features), bf16),
            pltpu.VMEM((1, features), f32),
            pltpu.VMEM((2, n, n, rows, features), bf16),
            pltpu.VMEM((features, tokens), f32),
            pltpu.VMEM((features, tokens), f32),
            pltpu.VMEM((features, tokens), f32),
            pltpu.VMEM((features, tokens), bf16),
            pltpu.VMEM((3, features, tokens), bf16),
            pltpu.VMEM((2, 8, tokens), f32),
            pltpu.VMEM((2, 2, tokens), f32),
            pltpu.VMEM((2, n, 2, tokens), f32),
            pltpu.VMEM((2, EARLY, 2, n) + block, f32),
            pltpu.VMEM((2, 2, EARLY, 2, 2) + block, f32),
            pltpu.VMEM((2, n, n) + block, f32),
            pltpu.VMEM((2, 2, n, half) + block, f32),
            pltpu.VMEM((2,) + block, f32),
            pltpu.VMEM((2, 2, half) + block, f32),
            pltpu.VMEM((2,) + block, f32),
            pltpu.VMEM((2, flips, 8, features), f32),
            pltpu.SemaphoreType.DMA((3 + 2 * n,)),
            pltpu.SemaphoreType.DMA((2, n)),
            pltpu.SemaphoreType.DMA((2, n)),
            pltpu.SemaphoreType.DMA((2, 2, EARLY, 2, 2)),
            pltpu.SemaphoreType.DMA((2, 2, EARLY, 2, 2)),
            pltpu.SemaphoreType.DMA((2, 2, n, half)),
            pltpu.SemaphoreType.DMA((2, 2, n, half)),
            pltpu.SemaphoreType.DMA((2, 2, half)),
            pltpu.SemaphoreType.DMA((2, 2, half)),
            pltpu.SemaphoreType.DMA((flips,)),
            pltpu.SemaphoreType.DMA((flips,)),
            pltpu.SemaphoreType.REGULAR((flips - 1,)),
        ],
        compiler_params=pltpu.CompilerParams(
            collective_id=0, has_side_effects=True, vmem_limit_bytes=60 * 1024 * 1024
        ),
        name="fused",
    )(grad_out, hidden_sum, norm_gain.reshape(1, features), out_weight.reshape(n, n, 2, rows, features))
    return out[:tokens], out[tokens:], gains.reshape(features)


def solution(mesh, n=8, zs=8):
    finer = Mesh(mesh.devices.reshape(n, n, zs, 2), ("y", "x", "z", "core"))
    tp, dp = ("y", "x"), ("z", "core")

    def whole(grad_out, hidden_sum, norm_gain, out_weight):
        return jax.shard_map(
            functools.partial(on_device, n, zs, grad_out.shape[1]),
            mesh=finer,
            in_specs=(P(dp, tp), P(dp, tp), P(tp), P(None, tp)),
            out_specs=(P(dp, tp), P(dp, tp), P(tp)),
            check_vma=False,
        )(grad_out, hidden_sum, norm_gain, out_weight)

    return whole
```

```python
import functools

import jax
import jax.numpy as jnp
from jax import lax
from jax.experimental import pallas as pl
from jax.experimental.pallas import tpu as pltpu
from jax.sharding import Mesh
from jax.sharding import PartitionSpec as P

EPSILON = 1e-05
MESH = pl.DeviceIdType.MESH
EARLY = 2


def kernel(
    n, width,
    grad_hbm, stream_hbm, gain_hbm, weight_hbm,
    out, gain_out,
    grad_v, stream_v, gain_v, weight_v,
    scaled_t, stream_t, resid_t, operand, early, token_v,
    stat, stat_in, early_part, early_ring, part, ring, turn, tail, final_t, gains,
    load_sem, stat_send, stat_recv, early_send, early_recv, ring_send, ring_recv, tail_send, tail_recv, gain_send, gain_recv, entered,
):
    y, x = lax.axis_index("y"), lax.axis_index("x")
    z, core = lax.axis_index("z"), lax.axis_index("core")
    half = n // 2
    here = {"x": x, "y": y}
    first_axis, second_axis = ("x", "y"), ("y", "x")
    rows = part.shape[-2]
    tokens = part.shape[-1]
    halved = rows // 2

    small = [
        pltpu.make_async_copy(s, d, load_sem.at[i])
        for i, (s, d) in enumerate(((grad_hbm, grad_v), (stream_hbm, stream_v), (gain_hbm, gain_v)))
    ]
    for load in small:
        load.start()
    def offset(c):
        c = jnp.int32(c)
        return lax.rem(lax.select(lax.rem(c, 2) == 1, (n - 1 - c) // 2, half + c // 2), n)

    def weight_load(h, c):
        i = lax.rem(here[second_axis[h]] + offset(c), n)
        return pltpu.make_async_copy(
            weight_hbm.at[i, :, 0] if h == 0 else weight_hbm.at[:, i, 1], weight_v.at[h, i], load_sem.at[3 + h * n + c]
        )

    for c in range(n):
        for h in range(2):
            weight_load(h, c).start()

    zs = lax.axis_size("z")
    flips, uppers, bit = [{"core": 1 - core}], [], 1
    while bit < zs:
        upper = lax.rem(z // bit, 2)
        flips.append({"z": z + bit - 2 * bit * upper})
        uppers.append(upper)
        bit *= 2
    barrier = pltpu.get_barrier_semaphore()
    peers = [{a: lax.rem(here[a] + j, n)} for a in ("x", "y") for j in range(1, n)] + flips[:1]
    for peer in peers:
        pl.semaphore_signal(barrier, inc=1, device_id=peer, device_id_type=MESH)
    for k, upper in enumerate(uppers):

        @pl.when(upper == 0)
        def _():
            pl.semaphore_signal(barrier, inc=1, device_id=flips[1 + k], device_id_type=MESH)

    for load in small:
        load.wait()
    grad = grad_v[...].astype(jnp.float32)
    stream = stream_v[...].astype(jnp.float32)
    scaled_t[...] = jnp.transpose(gain_v[...] * grad)
    stream_t[...] = jnp.transpose(stream)
    stat[0, 0:1, :] = jnp.sum(stream_t[...] * stream_t[...], axis=0, keepdims=True)
    stat[0, 1:2, :] = jnp.sum(scaled_t[...] * stream_t[...], axis=0, keepdims=True)
    scaled = scaled_t[...]
    high = scaled.astype(jnp.bfloat16)
    early[0] = high
    early[1] = (scaled - high.astype(jnp.float32)).astype(jnp.bfloat16)
    early[2] = stream_t[...].astype(jnp.bfloat16)
    pl.semaphore_wait(barrier, len(peers) + sum(uppers))

    def stat_copy(a, j):
        axis = ("x", "y")[a]
        return pltpu.make_async_remote_copy(
            src_ref=stat.at[a], dst_ref=stat_in.at[a, j],
            send_sem=stat_send.at[a, j], recv_sem=stat_recv.at[a, j],
            device_id={axis: lax.rem(here[axis] + j, n)}, device_id_type=MESH,
        )

    def spot(h, j):
        return lax.rem(here[first_axis[h]] + j, n)

    def slab(h, o):
        blocks = weight_v[h, lax.rem(here[second_axis[h]] + o, n)]
        return blocks.reshape(n * rows, blocks.shape[-1])

    def product(a, b):
        return jnp.dot(a, b, preferred_element_type=jnp.float32)

    def multiply(c):
        for h in range(2):
            part[h, c] = product(slab(h, offset(c)), operand[...]).reshape(n, rows, tokens)

    def multiply_early(c):
        for h in range(2):
            blocks = slab(h, offset(c))
            value = product(blocks, early[0]) + product(blocks, early[1])
            early_part[h, c, 0] = value.reshape(n, rows, tokens)
            early_part[h, c, 1] = product(blocks, early[2]).reshape(n, rows, tokens)

    def side(d):
        return pl.ds(d * halved, halved)

    def ring_copy(h, d, c, s):
        axis = first_axis[h]
        if s == 1:
            src, dst = part.at[h, c, spot(h, half), side(d)], ring.at[h, d, c, 0, side(d)]
        else:
            src, dst = ring.at[h, d, c, s - 2], ring.at[h, d, c, s - 1]
        return pltpu.make_async_remote_copy(
            src_ref=src, dst_ref=dst,
            send_sem=ring_send.at[h, d, c, s - 1], recv_sem=ring_recv.at[h, d, c, s - 1],
            device_id={axis: lax.rem(here[axis] + (1 if d == 0 else n - 1), n)}, device_id_type=MESH,
        )

    def tail_copy(h, d, s, last=False):
        axis = second_axis[h]
        if isinstance(s, int) and s == 1:
            src, dst = turn.at[h, side(d)], tail.at[h, d, 0, side(d)]
        else:
            src, dst = tail.at[h, d, s - 2], tail.at[h, d, s - 1]
        return pltpu.make_async_remote_copy(
            src_ref=src, dst_ref=dst,
            send_sem=tail_send.at[h, d, s - 1], recv_sem=tail_recv.at[h, d, s - 1],
            device_id={axis: lax.rem(here[axis] + 1 + d * (n - 2), n)}, device_id_type=MESH,
        )

    def begin(c):
        multiply(c)
        for h in range(2):
            for d in range(2):
                ring_copy(h, d, c, 1).start()

    def early_copy(h, d, c, g, s):
        axis = first_axis[h]
        if s == 1:
            src, dst = early_part.at[h, c, g, spot(h, half), side(d)], early_ring.at[h, d, c, g, 0, side(d)]
        else:
            src, dst = early_ring.at[h, d, c, g, 0], early_ring.at[h, d, c, g, 1]
        return pltpu.make_async_remote_copy(
            src_ref=src, dst_ref=dst,
            send_sem=early_send.at[h, d, c, g, s - 1], recv_sem=early_recv.at[h, d, c, g, s - 1],
            device_id={axis: lax.rem(here[axis] + (1 if d == 0 else n - 1), n)}, device_id_type=MESH,
        )

    def begin_early(c):
        multiply_early(c)
        for g in range(2):
            for h in range(2):
                for d in range(2):
                    early_copy(h, d, c, g, 1).start()

    def add(slot, other, d, s):
        if s == 1:
            slot[side(d)] += other[side(d)]
            slot[side(1 - d)] = other[side(1 - d)]
        else:
            slot[...] += other[...]

    def ahead(d, s):
        m = half + 1 - s
        return m if d == 0 else n - m

    def pass_on(c, s):
        for h in range(2):
            for d in range(2):
                ring_copy(h, d, c, s - 1).wait_recv()
                add(ring.at[h, d, c, s - 2], part.at[h, c, spot(h, ahead(d, s))], d, s - 1)
                ring_copy(h, d, c, s).start()

    def pass_early(c):
        for g in range(2):
            for h in range(2):
                for d in range(2):
                    early_copy(h, d, c, g, 1).wait_recv()
                    add(early_ring.at[h, d, c, g, 0], early_part.at[h, c, g, spot(h, ahead(d, 2))], d, 1)
                    early_copy(h, d, c, g, 2).start()

    def join_early(c):
        multiply(c)
        for h in range(2):
            for d in range(2):
                for g in range(2):
                    early_copy(h, d, c, g, 2).wait_recv()
                joined = early_ring[h, d, c, 0, 1] - early_ring[h, d, c, 1, 1] * token_v[1, 0:1]
                ring[h, d, c, 1] = token_v[0, 0:1] * joined + part[h, c, spot(h, ahead(d, 3))]
                ring_copy(h, d, c, 3).start()

    def sends_done(c, first=1, last=half):
        for h in range(2):
            for d in range(2):
                for s in range(first, last + 1):
                    ring_copy(h, d, c, s).wait_send()

    def gathered(h, e):
        for d in range(2):
            ring_copy(h, d, e, half).wait_recv()
        return ring[h, 0, e, half - 1] + ring[h, 1, e, half - 1] + part[h, e, spot(h, 0)]

    def turn_first():
        for h in range(2):
            turn[h] = gathered(h, 0)
            for d in range(2):
                tail_copy(h, d, 1).start()

    def arrive(c):
        for h in range(2):
            turn_value = gathered(h, c)
            d = 1 - lax.rem(c, 2)
            for s in range(2, half + 1):

                @pl.when(((c + 1) // 2 + 1 == s) & (c < n - 1))
                def _():
                    tail_copy(h, d, s - 1).wait_recv()
                    slot = tail.at[h, d, s - 2]
                    if s == 2:
                        other = pl.ds((1 - d) * halved, halved)
                        mine = part.at[h, c, spot(h, 0)]
                        mine[...] = turn_value
                        slot[side(d)] += mine[side(d)]
                        slot[other] = mine[other]
                    else:
                        slot[...] += turn_value
                    tail_copy(h, d, s).start()

            @pl.when(c == n - 1)
            def _():
                for d in range(2):
                    tail_copy(h, d, half).wait_recv()
                final_t[h] = turn_value + tail[h, 0, half - 1] + tail[h, 1, half - 1]

    def gain_copy(k):
        return pltpu.make_async_remote_copy(
            src_ref=gains.at[0, k], dst_ref=gains.at[1, k],
            send_sem=gain_send.at[k], recv_sem=gain_recv.at[k],
            device_id=flips[k], device_id_type=MESH,
        )

    def write_resid():
        out[0:tokens] = jnp.transpose(resid_t[...]).astype(out.dtype)

    def gain_first():
        column = jnp.transpose(jnp.broadcast_to(token_v[0, 0:1], (tokens, tokens)))
        gains[0, 0] = jnp.zeros_like(gains[0, 0])
        for i in range(grad_v.shape[1] // tokens):
            at = pl.ds(i * tokens, tokens)
            value = grad_v[:, at].astype(jnp.float32) * stream_v[:, at].astype(jnp.float32) * column
            gains[0, 0, 0:1, at] = jnp.sum(value, axis=0, keepdims=True)
        gain_copy(0).start()

    def gain_step(k):
        gain_copy(k - 1).wait_recv()
        gains[0, k] = gains[0, k - 1] + gains[1, k - 1]

        @pl.when(uppers[k - 1] == 0)
        def _():
            pl.semaphore_wait(entered.at[k - 1], 1)

        gain_copy(k).start()

    def send_stats(a):
        for j in sorted(range(1, n), key=lambda j: -min(j, n - j)):
            stat_copy(a, j).start()

    def take_stats(a):
        for j in sorted(range(1, n), key=lambda j: min(j, n - j)):
            stat_copy(a, j).wait_recv()
        both = stat[a]
        for j in range(1, n):
            both = both + stat_in[a, j]
        return both

    send_stats(0)
    for k, upper in enumerate(uppers):

        @pl.when(upper == 1)
        def _():
            pl.semaphore_signal(entered.at[k], inc=1, device_id=flips[1 + k], device_id_type=MESH)

    for c in range(EARLY):
        for h in range(2):
            weight_load(h, c).wait()
        begin_early(c)
    for c in range(EARLY, n):
        for h in range(2):
            weight_load(h, c).wait()
    stat[1] = take_stats(0)
    send_stats(1)
    middle = EARLY + (n - EARLY) // 2
    front, back = (EARLY, middle), (middle, n)

    def each(chunks, do):
        lax.fori_loop(chunks[0], chunks[1], lambda c, _: (do(c), 0)[1], 0)

    for c in range(EARLY):
        pass_early(c)
    both = take_stats(1)
    inverse = lax.rsqrt(both[0:1] / width + EPSILON)
    factor = inverse * inverse * both[1:2] / width
    token_v[0] = jnp.broadcast_to(inverse, token_v.shape[1:])
    token_v[1] = jnp.broadcast_to(factor, token_v.shape[1:])
    resid = inverse * (scaled_t[...] - stream_t[...] * factor)
    resid_t[...] = resid
    operand[...] = resid.astype(jnp.bfloat16)

    each(front, begin)
    each(back, begin)
    each((0, EARLY), join_early)
    gain_first()
    gain_step(1)
    each(front, lambda c: pass_on(c, 2))
    each((0, EARLY), lambda c: pass_on(c, 4))
    gain_step(2)
    each(front, lambda c: pass_on(c, 3))
    turn_first()
    each(front, lambda c: pass_on(c, 4))
    gain_step(3)
    write_resid()
    each((1, 3), arrive)
    each(back, lambda c: pass_on(c, 2))
    each((3, 5), arrive)
    each(back, lambda c: pass_on(c, 3))
    each((0, EARLY), lambda c: sends_done(c, 3))
    each(front, sends_done)
    for h in range(2):
        for d in range(2):
            for c in range(EARLY):
                for g in range(2):
                    for s in range(1, 3):
                        early_copy(h, d, c, g, s).wait_send()
    for a in range(2):
        for j in range(1, n):
            stat_copy(a, j).wait_send()
    for k in range(len(flips) - 1):
        gain_copy(k).wait_send()
    each(back, lambda c: pass_on(c, 4))
    each(back, lambda c: sends_done(c, 1, half - 1))
    for h in range(2):
        for d in range(2):
            for s in range(1, half):
                tail_copy(h, d, s).wait_send()
    each((5, n), arrive)

    for h in range(2):
        out[pl.ds(tokens, tokens), pl.ds(h * rows, rows)] = jnp.transpose(final_t[h]).astype(out.dtype)
    last = len(flips) - 1
    gain_copy(last).wait_recv()
    gain_out[...] = (gains[0, last] + gains[1, last])[0:1]

    each(back, lambda c: sends_done(c, half))
    for h in range(2):
        for d in range(2):
            tail_copy(h, d, half).wait_send()
    gain_copy(last).wait_send()


def on_device(n, zs, width, grad_out, hidden_sum, norm_gain, out_weight):
    tokens, features = grad_out.shape
    rows = features // 2
    half = n // 2
    flips = 1 + (zs - 1).bit_length()
    f32, bf16 = jnp.float32, jnp.bfloat16
    block = (rows, tokens)
    out, gains = pl.pallas_call(
        functools.partial(kernel, n, width),
        out_shape=(
            pltpu.VMEM((2 * tokens, features), bf16),
            pltpu.VMEM((1, features), f32),
        ),
        in_specs=[pl.BlockSpec(memory_space=pltpu.HBM)] * 4,
        out_specs=(pl.BlockSpec(memory_space=pltpu.VMEM),) * 2,
        scratch_shapes=[
            pltpu.VMEM((tokens, features), bf16),
            pltpu.VMEM((tokens, features), bf16),
            pltpu.VMEM((1, features), f32),
            pltpu.VMEM((2, n, n, rows, features), bf16),
            pltpu.VMEM((features, tokens), f32),
            pltpu.VMEM((features, tokens), f32),
            pltpu.VMEM((features, tokens), f32),
            pltpu.VMEM((features, tokens), bf16),
            pltpu.VMEM((3, features, tokens), bf16),
            pltpu.VMEM((2, 8, tokens), f32),
            pltpu.VMEM((2, 2, tokens), f32),
            pltpu.VMEM((2, n, 2, tokens), f32),
            pltpu.VMEM((2, EARLY, 2, n) + block, f32),
            pltpu.VMEM((2, 2, EARLY, 2, 2) + block, f32),
            pltpu.VMEM((2, n, n) + block, f32),
            pltpu.VMEM((2, 2, n, half) + block, f32),
            pltpu.VMEM((2,) + block, f32),
            pltpu.VMEM((2, 2, half) + block, f32),
            pltpu.VMEM((2,) + block, f32),
            pltpu.VMEM((2, flips, 8, features), f32),
            pltpu.SemaphoreType.DMA((3 + 2 * n,)),
            pltpu.SemaphoreType.DMA((2, n)),
            pltpu.SemaphoreType.DMA((2, n)),
            pltpu.SemaphoreType.DMA((2, 2, EARLY, 2, 2)),
            pltpu.SemaphoreType.DMA((2, 2, EARLY, 2, 2)),
            pltpu.SemaphoreType.DMA((2, 2, n, half)),
            pltpu.SemaphoreType.DMA((2, 2, n, half)),
            pltpu.SemaphoreType.DMA((2, 2, half)),
            pltpu.SemaphoreType.DMA((2, 2, half)),
            pltpu.SemaphoreType.DMA((flips,)),
            pltpu.SemaphoreType.DMA((flips,)),
            pltpu.SemaphoreType.REGULAR((flips - 1,)),
        ],
        compiler_params=pltpu.CompilerParams(
            collective_id=0, has_side_effects=True, vmem_limit_bytes=60 * 1024 * 1024
        ),
        name="fused",
    )(grad_out, hidden_sum, norm_gain.reshape(1, features), out_weight.reshape(n, n, 2, rows, features))
    return out[:tokens], out[tokens:], gains.reshape(features)


def solution(mesh, n=8, zs=8):
    finer = Mesh(mesh.devices.reshape(n, n, zs, 2), ("y", "x", "z", "core"))
    tp, dp = ("y", "x"), ("z", "core")

    def whole(grad_out, hidden_sum, norm_gain, out_weight):
        return jax.shard_map(
            functools.partial(on_device, n, zs, grad_out.shape[1]),
            mesh=finer,
            in_specs=(P(dp, tp), P(dp, tp), P(tp), P(None, tp)),
            out_specs=(P(dp, tp), P(dp, tp), P(tp)),
            check_vma=False,
        )(grad_out, hidden_sum, norm_gain, out_weight)

    return whole
```
